32 devices in a mesh: row: 16 (over z, y, core), col: 2 (over x).
Axes of the slice: x: 2, y: 2, z: 4, core: 2. Of those that a mesh axis runs over, the one named last changes fastest.
Arguments:
- pair: bfloat16 [256, 256, 128], P('row', 'col'), may hold values from -6 to 6
- relpos: bfloat16 [128, 128], replicated, may hold values from -4 to 4
- pair_gain: float32 [128], replicated, may hold values from 0.1 to 1.9
- bias_weight: bfloat16 [128, 12], replicated, may hold values from -0.5 to 0.5
- single: float32 [256, 384], P(('row', 'col')), may hold values from -6 to 6
- rotation_params: float32 [3, 256], P(None, ('row', 'col')), may hold values from -4 to 4
- translation: float32 [3, 256], P(None, ('row', 'col')), may hold values from -9 to 9
- residue_index: int32 [256], P(('row', 'col')), may hold values from 0 to 50944, as said below
- residue_mask: int32 [256], P(('row', 'col')), may hold values 0 or 1
- w_scalar: float32 [384, 576], replicated, may hold values from -0.3125 to 0.3125
- w_points: float32 [384, 576], replicated, may hold values from -0.3125 to 0.3125
- head_weights: float32 [12], replicated, may hold values from -2 to 1.5
- w_out: float32 [2112, 384], replicated, may hold values from -0.125 to 0.125
- w_hidden: float32 [384, 384], replicated, may hold values from -0.3125 to 0.3125
- w_back: float32 [384, 384], replicated, may hold values from -0.3125 to 0.3125
- w_frame: float32 [384, 6], replicated, may hold values from -0.078125 to 0.078125
Outputs:
- single_out: float32 [256, 384], P(('row', 'col'))
- frames: float32 [12, 256], P(None, ('row', 'col'))
The draws below stay inside these ranges and needn't reach their ends.
Inputs may be any that keep to these rules, and one draw needn't show every extreme that they name: residue_index is strictly increasing along the crop, begins at 0 and ends at exactly 50944.
All inputs are finite; a program needn't handle non-finite values. No bound on the sum of `residue_mask` on one device may be relied on, other than what follows from the above.
Results may differ from the reference program's by a relative error of at most 0.0025.
Values may be sent and summed in bfloat16 or wider, within the bound.
A program may use at most 64 MiB of HBM per device.

```python
import math
import jax
import jax.numpy as jnp
from jax import lax

D = 384
CZ = 128
H = 12
C = 16
PQ = 4
PV = 8
BINS = 128
ITERS = 3
N = 256
OUT_F = 2112


def draw_residue_index(key, part):
    key_step, key_break, key_jump = jax.random.split(jax.random.fold_in(key, 17), 3)
    steps = jax.random.randint(key_step, (N,), 1, 3)
    breaks = jax.random.randint(key_break, (N,), 0, 64) == 0
    jumps = jax.random.randint(key_jump, (N,), 50, 200)
    steps = jnp.where(breaks, jumps, steps)
    numbers = (jnp.cumsum(steps) - steps[0]).astype(jnp.int32)
    position = jnp.arange(N, dtype=jnp.int32)
    return jnp.where(position == N - 1, jnp.int32(199 * N), numbers).astype(jnp.int32)


def plant(values, key, least, top_value):
    index_at = [jax.random.randint(jax.random.fold_in(key, axis), (), 0, length) for axis, length in enumerate(values.shape)]
    main_axis = values.shape.index(max(values.shape))
    next_to = index_at[:main_axis] + [(index_at[main_axis] + 1) % values.shape[main_axis]] + index_at[main_axis + 1:]
    return values.at[tuple(index_at)].set(least).at[tuple(next_to)].set(top_value)


def block_scale(stream_key, dims, pieces, least, high):
    loudness, own = 1.0, jax.random.fold_in(stream_key, 6)
    for axis_at, blocks in pieces:
        heights = jnp.exp(jax.random.uniform(jax.random.fold_in(own, axis_at), (blocks,), jnp.float32, least / len(pieces), high / len(pieces)))
        loudness = loudness * jnp.repeat(heights, dims[axis_at] // blocks).reshape([-1 if axis == axis_at else 1 for axis in range(len(dims))])
    return loudness


def bell_draw(own_key, shape, scale, most, pieces=(), kind=jnp.bfloat16):
    values = jax.random.normal(own_key, shape, jnp.float32) * scale
    if len(pieces) > 0:
        values = block_scale(own_key, shape, pieces, -0.22, 0.18) * values
    return jnp.clip(values, min=-most, max=most).astype(kind)


def setup_inputs(seed: int = 0) -> dict:
    key_of = jax.random.split(jax.random.key(seed), 17)
    pair = bell_draw(key_of[0], (N, N, CZ), 1.0, 6.0, ((0, 16), (1, 2)))
    relpos = bell_draw(key_of[1], (BINS, CZ), 0.7, 4.0)
    pair_gain = jnp.clip(1.0 + 0.18 * jax.random.normal(key_of[2], (CZ,), jnp.float32), 0.1, 1.9)
    bias_weight = bell_draw(key_of[3], (CZ, H), CZ ** -0.5, 0.5)
    single = bell_draw(key_of[4], (N, D), 1.0, 6.0, ((0, 32),), jnp.float32)
    rotation_params = bell_draw(key_of[5], (3, N), 0.7, 4.0, ((1, 32),), jnp.float32)
    translation = bell_draw(key_of[6], (3, N), 1.5, 9.0, ((1, 32),), jnp.float32)
    residue_index = draw_residue_index(jax.random.fold_in(key_of[16], 71), 0)
    residue_mask = plant((jax.random.randint(key_of[8], (N,), 0, 8) < 7).astype(jnp.int32), jax.random.fold_in(key_of[8], 1), 0, 1)
    w_scalar = bell_draw(key_of[9], (D, 3 * H * C), D ** -0.5, 0.3125, (), jnp.float32)
    w_points = bell_draw(key_of[10], (D, 3 * H * (2 * PQ + PV)), D ** -0.5, 0.3125, (), jnp.float32)
    head_weights = jnp.clip(jax.random.uniform(key_of[11], (H,), jnp.float32, -2.0, 1.5), -2.0, 1.5)
    w_out = bell_draw(key_of[12], (OUT_F, D), OUT_F ** -0.5, 0.125, (), jnp.float32)
    w_hidden = bell_draw(key_of[13], (D, D), D ** -0.5, 0.3125, (), jnp.float32)
    w_back = bell_draw(key_of[14], (D, D), D ** -0.5, 0.3125, (), jnp.float32)
    w_frame = bell_draw(key_of[15], (D, 6), (16 * D) ** -0.5, 0.078125, (), jnp.float32)
    return dict(pair=pair, relpos=relpos, pair_gain=pair_gain, bias_weight=bias_weight, single=single, rotation_params=rotation_params, translation=translation, residue_index=residue_index, residue_mask=residue_mask, w_scalar=w_scalar, w_points=w_points, head_weights=head_weights, w_out=w_out, w_hidden=w_hidden, w_back=w_back, w_frame=w_frame)


NORM_EPSILON = 1e-05
MASKED_LOGIT = -100000.0
NORM_FLOOR = 0.1
HIGHEST_PRECISION = lax.Precision.HIGHEST

def layer_norm(values):
    center = values - lax.optimization_barrier(jnp.mean(values, axis=-1, keepdims=True))
    spread = lax.optimization_barrier(jnp.mean(center * center, axis=-1, keepdims=True))
    return center * lax.rsqrt(spread + NORM_EPSILON)

def rotation_from(update):
    quat_b, quat_c, quat_d = (update[0], update[1], update[2])
    inverse = 1.0 / (1.0 + quat_b * quat_b + quat_c * quat_c + quat_d * quat_d)
    entries = [1.0 + quat_b * quat_b - quat_c * quat_c - quat_d * quat_d, 2.0 * (quat_b * quat_c - quat_d), 2.0 * (quat_b * quat_d + quat_c), 2.0 * (quat_b * quat_c + quat_d), 1.0 - quat_b * quat_b + quat_c * quat_c - quat_d * quat_d, 2.0 * (quat_c * quat_d - quat_b), 2.0 * (quat_b * quat_d - quat_c), 2.0 * (quat_c * quat_d + quat_b), 1.0 - quat_b * quat_b - quat_c * quat_c + quat_d * quat_d]
    return jnp.stack(entries) * inverse

def to_global(rotation, points, translation):
    return jnp.stack([rotation[3 * component] * points[0] + rotation[3 * component + 1] * points[1] + rotation[3 * component + 2] * points[2] + translation[component] for component in range(3)])

def to_local(rotation, points, translation):
    moved = [points[component] - translation[component] for component in range(3)]
    return jnp.stack([rotation[component] * moved[0] + rotation[3 + component] * moved[1] + rotation[6 + component] * moved[2] for component in range(3)])

def compose(rotation, translation, update):
    turn = rotation_from(update[:3])
    new_rotation = jnp.stack([rotation[3 * left] * turn[right] + rotation[3 * left + 1] * turn[3 + right] + rotation[3 * left + 2] * turn[6 + right] for left in range(3) for right in range(3)])
    new_translation = jnp.stack([rotation[3 * left] * update[3] + rotation[3 * left + 1] * update[4] + rotation[3 * left + 2] * update[5] + translation[left] for left in range(3)])
    return (new_rotation, new_translation)

def project(single, rotation, translation, w_scalar, w_points):
    count = single.shape[0]
    scalars = jnp.dot(single, w_scalar, precision=HIGHEST_PRECISION, preferred_element_type=jnp.float32).T
    scalars = scalars.reshape(3, H * C, count).astype(jnp.bfloat16)
    points = jnp.dot(single, w_points, precision=HIGHEST_PRECISION, preferred_element_type=jnp.float32).T
    query_local = points[:3 * H * PQ].reshape(3, H * PQ, count)
    key_local = points[3 * H * PQ:6 * H * PQ].reshape(3, H * PQ, count)
    value_local = points[6 * H * PQ:].reshape(3, H * PV, count)
    return (scalars, to_global(rotation, query_local, translation), to_global(rotation, key_local, translation), to_global(rotation, value_local, translation))

def advance(single, rotation, translation, scalar_out, point_out, pair_out, w_out, w_hidden, w_back, w_frame):
    count = single.shape[0]
    local = to_local(rotation, point_out, translation)
    lengths = jnp.sqrt(lax.optimization_barrier(jnp.sum(local * local, axis=0)) + NORM_FLOOR)
    features = jnp.concatenate([scalar_out, local.reshape(3 * H * PV, count), lengths, pair_out], axis=0)
    single = layer_norm(single + jnp.dot(features.T, w_out, precision=HIGHEST_PRECISION, preferred_element_type=jnp.float32))
    hidden = jax.nn.relu(jnp.dot(single, w_hidden, precision=HIGHEST_PRECISION, preferred_element_type=jnp.float32))
    single = layer_norm(single + jnp.dot(hidden, w_back, precision=HIGHEST_PRECISION, preferred_element_type=jnp.float32))
    update = jnp.dot(single, w_frame, precision=HIGHEST_PRECISION, preferred_element_type=jnp.float32).T
    rotation, translation = compose(rotation, translation, update)
    return (single, rotation, translation)

def reference(pair, relpos, pair_gain, bias_weight, single, rotation_params, translation, residue_index, residue_mask, w_scalar, w_points, head_weights, w_out, w_hidden, w_back, w_frame):
    span_rows = math.gcd(N, 128)
    count = N // span_rows
    live = residue_mask == 1
    table = relpos.astype(jnp.float32)
    point_scale = jax.nn.softplus(head_weights) * (math.sqrt(2.0 / (9.0 * PQ)) / 2.0)

    def prepare(index):
        start = index * span_rows
        rows = lax.dynamic_slice_in_dim(pair, start, span_rows, 0).astype(jnp.float32)
        near = lax.dynamic_slice_in_dim(residue_index, start, span_rows, 0)
        offset = jnp.clip(residue_index[None, :] - near[:, None], -(BINS // 2), BINS // 2 - 1) + BINS // 2
        normed = (layer_norm(rows + table[offset]) * pair_gain).astype(jnp.bfloat16)
        bias = jnp.einsum('ijc,ch->hij', normed.astype(jnp.float32), bias_weight.astype(jnp.float32), precision=HIGHEST_PRECISION)
        return (normed, bias)
    rotation = rotation_from(rotation_params)
    state = single
    for step in range(ITERS):
        scalars, query_points, key_points, value_points = project(state, rotation, translation, w_scalar, w_points)
        query = scalars[0].reshape(H, C, N)
        keys = scalars[1].reshape(H, C, N).astype(jnp.float32)
        values = scalars[2].reshape(H, C, N).astype(jnp.float32)
        query_grid = query_points.reshape(3, H, PQ, N)
        key_grid = key_points.reshape(3, H, PQ, N)
        value_grid = value_points.reshape(3, H, PV, N)
        key_square = lax.optimization_barrier(jnp.sum(key_grid * key_grid, axis=(0, 2)))

        def attend(index):
            normed, bias = prepare(index)
            start = index * span_rows
            query_block = lax.dynamic_slice_in_dim(query, start, span_rows, 2).astype(jnp.float32)
            query_block_points = lax.dynamic_slice_in_dim(query_grid, start, span_rows, 3)
            scores = jnp.einsum('hci,hcj->hij', query_block, keys, precision=HIGHEST_PRECISION) / math.sqrt(C)
            cross = jnp.einsum('ahpi,ahpj->hij', query_block_points, key_grid, precision=HIGHEST_PRECISION)
            distance = lax.optimization_barrier(jnp.sum(query_block_points * query_block_points, axis=(0, 2)))[:, :, None] + key_square[:, None, :] - 2.0 * cross
            logits = math.sqrt(1.0 / 3.0) * (scores + bias - point_scale[:, None, None] * distance)
            live_block = lax.dynamic_slice_in_dim(live, start, span_rows, 0)
            logits = jnp.where(live_block[None, :, None] & live[None, None, :], logits, MASKED_LOGIT)
            weights = jax.nn.softmax(logits, axis=-1)
            rounded = lax.optimization_barrier(weights.astype(jnp.bfloat16)).astype(jnp.float32)
            scalar_part = jnp.einsum('hij,hcj->hci', rounded, values, precision=HIGHEST_PRECISION)
            point_part = jnp.einsum('hij,ahpj->ahpi', weights, value_grid, precision=HIGHEST_PRECISION)
            pair_part = jnp.einsum('hij,ijc->hci', rounded, normed.astype(jnp.float32), precision=HIGHEST_PRECISION)
            return (scalar_part.reshape(H * C, span_rows), point_part.reshape(3 * H * PV, span_rows), pair_part.reshape(H * CZ, span_rows))
        scalar_part, point_part, pair_part = lax.map(attend, jnp.arange(count, dtype=jnp.int32))
        scalar_out = scalar_part.transpose(1, 0, 2).reshape(H * C, N)
        point_out = point_part.transpose(1, 0, 2).reshape(3, H * PV, N)
        pair_out = pair_part.transpose(1, 0, 2).reshape(H * CZ, N)
        state, rotation, translation = advance(state, rotation, translation, scalar_out, point_out, pair_out, w_out, w_hidden, w_back, w_frame)
    frames = jnp.concatenate([rotation, translation], axis=0)
    return (state, frames)
```

```python
import functools
import math

import jax
import jax.numpy as jnp
from jax import lax
from jax.experimental import pallas as pl
from jax.experimental.pallas import tpu as pltpu
from jax.sharding import PartitionSpec as P

H = 12
HP = 16
C = 16
PQ = 4
PV = 8
BINS = 128
ITERS = 3
D = 384
WIDE = 512
NORM_EPSILON = 1e-05
MASKED_LOGIT = -100000.0
NORM_FLOOR = 0.1
MESH = pl.DeviceIdType.MESH
F32 = jnp.float32
BF16 = jnp.bfloat16
NN = (((1,), (0,)), ((), ()))
NT = (((1,), (1,)), ((), ()))
INDEX_AT = 12
MASK_AT = 13


def rotation_from(quat_b, quat_c, quat_d):
    inverse = 1.0 / (1.0 + quat_b * quat_b + quat_c * quat_c + quat_d * quat_d)
    entries = [
        1.0 + quat_b * quat_b - quat_c * quat_c - quat_d * quat_d,
        2.0 * (quat_b * quat_c - quat_d),
        2.0 * (quat_b * quat_d + quat_c),
        2.0 * (quat_b * quat_c + quat_d),
        1.0 - quat_b * quat_b + quat_c * quat_c - quat_d * quat_d,
        2.0 * (quat_c * quat_d - quat_b),
        2.0 * (quat_b * quat_d - quat_c),
        2.0 * (quat_c * quat_d + quat_b),
        1.0 - quat_b * quat_b - quat_c * quat_c + quat_d * quat_d,
    ]
    return [entry * inverse for entry in entries]


def layer_norm(values):
    center = values - jnp.mean(values, axis=-1, keepdims=True)
    spread = jnp.mean(center * center, axis=-1, keepdims=True)
    return center * lax.rsqrt(spread + NORM_EPSILON)


def split(x):
    high = x.astype(BF16)
    return high, (x - high.astype(F32)).astype(BF16)


def mm(a, b, dims=NN):
    return lax.dot_general(a, b, dims, preferred_element_type=F32)


def mm3(a, b, dims=NN):
    return mm(a[0], b[0], dims) + (mm(a[0], b[1], dims) + mm(a[1], b[0], dims))


def head_mask(width):
    head = lax.broadcasted_iota(jnp.int32, (HP, H * width), 0) * width
    lane = lax.broadcasted_iota(jnp.int32, (HP, H * width), 1)
    return ((lane >= head) & (lane < head + width)).astype(F32)


def spread_heads(rows, mask):
    return jnp.concatenate(
        [rows[i : i + 1] * mask for i in range(rows.shape[0])], axis=0
    )


def pick_heads(rows, mask):
    width = rows.shape[1]
    return jnp.sum(rows.reshape(-1, HP, width) * mask[None], axis=1)


def kernel(
    nrow,
    ncol,
    s0_ref,
    pair_ref,
    relpos_ref,
    gain_ref,
    bw_ref,
    ps_ref,
    ws_ref,
    wp_ref,
    wo_ref,
    wh_ref,
    wb_ref,
    wf_ref,
    single_ref,
    frames_ref,
    state,
    gathered,
    pairs,
    normed,
    bias,
    pair_out,
    wst,
    wpt,
    wo2,
    wh2,
    wb2,
    pair_send,
    pair_recv,
    pair_local,
    state_send,
    state_recv,
):
    n = nrow * ncol
    row = lax.axis_index("row")
    col = lax.axis_index("col")
    me = row * ncol + col
    owned = s0_ref.shape[0]
    count = n * owned
    col_rows = pair_ref.shape[1]

    barrier = pltpu.get_barrier_semaphore()

    def greet(k, carry):
        other = lax.rem(me + k, n)
        pl.semaphore_signal(
            barrier, inc=1, device_id=(other // ncol, lax.rem(other, ncol)), device_id_type=MESH
        )
        return carry

    lax.fori_loop(1, n, greet, 0)

    my_rows = pl.ds(pl.multiple_of(me * owned, owned), owned)
    my_cols = pl.ds(pl.multiple_of(col * col_rows, col_rows), col_rows)

    def state_copy(step, k):
        other = lax.rem(me + k, n)
        return pltpu.make_async_remote_copy(
            src_ref=state.at[step],
            dst_ref=gathered.at[step, my_rows],
            send_sem=state_send.at[step],
            recv_sem=state_recv.at[step],
            device_id=(other // ncol, lax.rem(other, ncol)),
            device_id_type=MESH,
        )

    def send_state(step):
        def one(k, carry):
            state_copy(step, k).start()
            return carry

        lax.fori_loop(1, n, one, 0)

    def wait_all(step, sem):
        part = gathered.at[step, pl.ds(0, (n - 1) * owned)]
        pltpu.make_async_copy(part, part, sem.at[step]).wait()

    state[0] = s0_ref[...]
    gathered[0, my_rows] = s0_ref[...]
    own_pair = pltpu.make_async_copy(
        pair_ref.at[pl.ds(col * owned, owned)], pairs.at[:, my_cols], pair_local
    )
    own_pair.start()
    pl.semaphore_wait(barrier, n - 1)
    send_state(0)
    for k in range(1, ncol):
        other = lax.rem(col + k, ncol)
        pltpu.make_async_remote_copy(
            src_ref=pair_ref.at[pl.ds(other * owned, owned)],
            dst_ref=pairs.at[:, my_cols],
            send_sem=pair_send,
            recv_sem=pair_recv,
            device_id=(row, other),
            device_id_type=MESH,
        ).start()

    for source, target in ((ws_ref, wst), (wp_ref, wpt)):
        total = source.shape[1]
        for begin in range(0, total, 128):
            end = min(begin + 128, total)
            high, low = split(source[:, begin:end].T)
            target[0, begin:end] = high
            target[1, begin:end] = low
    for source, target in ((wo_ref, wo2), (wh_ref, wh2), (wb_ref, wb2)):
        high, low = split(source[...])
        target[0] = high
        target[1] = low

    own_pair.wait()
    if ncol > 1:
        part = pairs.at[:, pl.ds(0, (ncol - 1) * col_rows)]
        pltpu.make_async_copy(part, part, pair_recv).wait()
    wait_all(0, state_recv)

    index_col = gathered[0, :, D : D + 128][:, INDEX_AT : INDEX_AT + 1]
    lanes = lax.broadcasted_iota(jnp.int32, (count, BINS), 1).astype(F32)
    own_index = s0_ref[:, D:][:, INDEX_AT : INDEX_AT + 1]
    sublanes = lax.broadcasted_iota(jnp.int32, (owned, 1), 0)
    relpos = relpos_ref[...]
    gain = gain_ref[...]
    bw = bw_ref[...]

    def prepare(i, carry):
        mine = jnp.sum(jnp.where(sublanes == i, own_index, 0.0), axis=0, keepdims=True)
        offset = jnp.clip(index_col - mine, -(BINS // 2), BINS // 2 - 1) + BINS // 2
        onehot = (offset == lanes).astype(F32).astype(BF16)
        summed = pairs[i].astype(F32) + mm(onehot, relpos)
        rows = (layer_norm(summed) * gain).astype(BF16)
        normed[i] = rows
        bias[i] = mm(bw, rows, NT)
        return carry

    lax.fori_loop(0, owned, prepare, 0)

    def dense(x, weight, begin, size):
        high, low = split(x)
        stacked = jnp.concatenate([high.astype(F32), low.astype(F32)], axis=0).astype(BF16)
        both = mm(stacked, weight[0, begin : begin + size])
        return both[:owned] + both[owned:] + mm(high, weight[1, begin : begin + size])

    def step_body(step, carry):
        @pl.when(step > 0)
        def _():
            wait_all(step, state_recv)

        turned = gathered[step].T
        x = split(turned[:D])
        frame = [turned[D + k : D + k + 1] for k in range(14)]
        mine = state[step]
        own = mine[:, :D]
        block = mine[:, D:]
        rot = [block[:, k : k + 1] for k in range(9)]
        pos = [block[:, 9 + k : 10 + k] for k in range(3)]
        own2 = split(own)
        hc = H * C
        keyval = mm3((wst[0, hc:], wst[1, hc:]), x).astype(BF16)
        keys, values = keyval[:hc], keyval[hc:]
        kp = 3 * H * PQ
        locals_t = mm3((wpt[0, kp:], wpt[1, kp:]), x)

        def lift(base, width):
            p = [locals_t[base + a * width : base + (a + 1) * width] for a in range(3)]
            return [
                frame[3 * a] * p[0] + frame[3 * a + 1] * p[1] + frame[3 * a + 2] * p[2] + frame[9 + a]
                for a in range(3)
            ]

        key_points = lift(0, H * PQ)
        value_points = lift(kp, H * PV)
        query = mm3(own2, (wst[0, :hc], wst[1, :hc]), NT).astype(BF16).astype(F32)
        q = [
            mm3(
                own2,
                (
                    wpt[0, a * H * PQ : (a + 1) * H * PQ],
                    wpt[1, a * H * PQ : (a + 1) * H * PQ],
                ),
                NT,
            )
            for a in range(3)
        ]
        query_points = [
            rot[3 * a] * q[0] + rot[3 * a + 1] * q[1] + rot[3 * a + 2] * q[2] + pos[a]
            for a in range(3)
        ]
        mask_c, mask_q, mask_v = head_mask(C), head_mask(PQ), head_mask(PV)
        scores = mm(spread_heads(query, mask_c).astype(BF16), keys) * (1.0 / math.sqrt(C))
        cross = None
        query_square = None
        for a in range(3):
            wide = spread_heads(query_points[a], mask_q)
            term = mm3(split(wide), split(key_points[a]))
            square = jnp.sum(wide * wide, axis=-1, keepdims=True)
            cross = term if cross is None else cross + term
            query_square = square if query_square is None else query_square + square
        squares = (
            key_points[0] * key_points[0]
            + key_points[1] * key_points[1]
            + key_points[2] * key_points[2]
        )
        selector = jnp.concatenate([mask_q] * owned, axis=0).astype(BF16)
        square_high, square_low = split(squares)
        square_rest = (squares - square_high.astype(F32) - square_low.astype(F32)).astype(BF16)
        key_square = mm(selector, square_high) + (
            mm(selector, square_low) + mm(selector, square_rest)
        )
        distance = query_square + key_square - 2.0 * cross
        biases = bias[...].reshape(owned * HP, count)
        logits = math.sqrt(1.0 / 3.0) * (scores + biases - ps_ref[...] * distance)
        ones = jnp.ones((HP, 1), F32)
        live_row = jnp.concatenate(
            [block[i : i + 1, MASK_AT : MASK_AT + 1] * ones for i in range(owned)], axis=0
        )
        logits = jnp.where(live_row * frame[MASK_AT] > 0.5, logits, MASKED_LOGIT)
        top = jnp.max(logits, axis=-1, keepdims=True)
        weights = jnp.exp(logits - top)
        weights = weights * (1.0 / jnp.sum(weights, axis=-1, keepdims=True))
        weights2 = split(weights)
        rounded = weights2[0]
        scalar_out = pick_heads(mm(rounded, values, NT), mask_c)
        for i in range(owned):
            pair_out[i] = mm(rounded[i * HP : (i + 1) * HP], normed[i])
        moved = [
            pick_heads(mm3(weights2, split(value_points[a]), NT), mask_v) - pos[a]
            for a in range(3)
        ]
        local = [rot[a] * moved[0] + rot[3 + a] * moved[1] + rot[6 + a] * moved[2] for a in range(3)]
        lengths = jnp.sqrt(
            local[0] * local[0] + local[1] * local[1] + local[2] * local[2] + NORM_FLOOR
        )
        pv = H * PV
        mixed = dense(scalar_out, wo2, 0, hc)
        for a in range(3):
            mixed = mixed + dense(local[a], wo2, hc + a * pv, pv)
        mixed = mixed + dense(lengths, wo2, hc + 3 * pv, pv)
        pairs_flat = jnp.concatenate([pair_out[:, h, :] for h in range(H)], axis=-1)
        begin = hc + 4 * pv
        mixed = mixed + dense(pairs_flat, wo2, begin, H * BINS)
        single = layer_norm(own + mixed)
        hidden = jnp.maximum(dense(single, wh2, 0, D), 0.0)
        single = layer_norm(single + dense(hidden, wb2, 0, D))
        update = mm3(split(single), split(wf_ref[...]))
        u = [update[:, k : k + 1] for k in range(6)]
        turn = rotation_from(u[0], u[1], u[2])
        new_rot = [
            rot[3 * a] * turn[b] + rot[3 * a + 1] * turn[3 + b] + rot[3 * a + 2] * turn[6 + b]
            for a in range(3)
            for b in range(3)
        ]
        new_pos = [
            rot[3 * a] * u[3] + rot[3 * a + 1] * u[4] + rot[3 * a + 2] * u[5] + pos[a]
            for a in range(3)
        ]
        place = lax.broadcasted_iota(jnp.int32, (owned, 128), 1)
        packed = block
        for k, entry in enumerate(new_rot + new_pos):
            packed = jnp.where(place == k, entry, packed)
        state[step + 1, :, :D] = single
        state[step + 1, :, D:] = packed

        @pl.when(step < ITERS - 1)
        def _():
            send_state(step + 1)
            gathered[step + 1, my_rows, :D] = single
            gathered[step + 1, my_rows, D:] = packed

        return carry

    lax.fori_loop(0, ITERS, step_body, 0)
    single_ref[...] = state[ITERS, :, :D]
    frames_ref[...] = state[ITERS, :, D:]
    for step in range(ITERS):
        wait_all(step, state_send)
    if ncol > 1:
        part = pairs.at[:, pl.ds(0, (ncol - 1) * col_rows)]
        pltpu.make_async_copy(part, part, pair_send).wait()


def body(
    nrow,
    ncol,
    pair,
    relpos,
    pair_gain,
    bias_weight,
    single,
    rotation_params,
    translation,
    residue_index,
    residue_mask,
    w_scalar,
    w_points,
    head_weights,
    w_out,
    w_hidden,
    w_back,
    w_frame,
):
    owned = single.shape[0]
    count = owned * nrow * ncol
    channels = pair.shape[2]
    out_f = w_out.shape[0]
    rotation = jnp.stack(rotation_from(*rotation_params))
    extra = jnp.concatenate(
        [
            rotation,
            translation,
            residue_index[None].astype(F32),
            residue_mask[None].astype(F32),
            jnp.zeros((WIDE - D - 14, owned), F32),
        ],
        axis=0,
    )
    s0 = jnp.concatenate([single, extra.T], axis=1)
    point_scale = jax.nn.softplus(head_weights) * (math.sqrt(2.0 / (9.0 * PQ)) / 2.0)
    ps = jnp.tile(jnp.pad(point_scale, (0, HP - H)), owned)[:, None]
    bw = jnp.pad(bias_weight.T, ((0, HP - H), (0, 0)))
    vmem = pl.BlockSpec(memory_space=pltpu.VMEM)
    out, frames = pl.pallas_call(
        functools.partial(kernel, nrow, ncol),
        out_shape=(
            jax.ShapeDtypeStruct((owned, D), F32),
            jax.ShapeDtypeStruct((owned, WIDE - D), F32),
        ),
        in_specs=[vmem] * 12,
        out_specs=(vmem, vmem),
        scratch_shapes=[
            pltpu.VMEM((ITERS + 1, owned, WIDE), F32),
            pltpu.VMEM((ITERS, count, WIDE), F32),
            pltpu.VMEM((owned, count, channels), BF16),
            pltpu.VMEM((owned, count, channels), BF16),
            pltpu.VMEM((owned, HP, count), F32),
            pltpu.VMEM((owned, HP, channels), F32),
            pltpu.VMEM((2, w_scalar.shape[1], D), BF16),
            pltpu.VMEM((2, w_points.shape[1], D), BF16),
            pltpu.VMEM((2, out_f, D), BF16),
            pltpu.VMEM((2, D, D), BF16),
            pltpu.VMEM((2, D, D), BF16),
            pltpu.SemaphoreType.DMA,
            pltpu.SemaphoreType.DMA,
            pltpu.SemaphoreType.DMA,
            pltpu.SemaphoreType.DMA((ITERS,)),
            pltpu.SemaphoreType.DMA((ITERS,)),
        ],
        compiler_params=pltpu.CompilerParams(
            collective_id=0, has_side_effects=True, vmem_limit_bytes=58 * 1024 * 1024
        ),
    )(
        s0, pair, relpos, pair_gain[None], bw, ps, w_scalar, w_points, w_out, w_hidden, w_back, w_frame
    )
    return out, frames[:, :12].T


def solution(mesh):
    placed = (
        P("row", "col", None),
        P(),
        P(),
        P(),
        P(("row", "col"), None),
        P(None, ("row", "col")),
        P(None, ("row", "col")),
        P(("row", "col")),
        P(("row", "col")),
        P(),
        P(),
        P(),
        P(),
        P(),
        P(),
        P(),
    )
    return jax.shard_map(
        functools.partial(body, mesh.shape["row"], mesh.shape["col"]),
        mesh=mesh,
        in_specs=placed,
        out_specs=(P(("row", "col"), None), P(None, ("row", "col"))),
        check_vma=False,
    )
```

```python
import functools
import math

import jax
import jax.numpy as jnp
from jax import lax
from jax.experimental import pallas as pl
from jax.experimental.pallas import tpu as pltpu
from jax.sharding import PartitionSpec as P

H = 12
HP = 16
C = 16
PQ = 4
PV = 8
BINS = 128
ITERS = 3
D = 384
WIDE = 512
NORM_EPSILON = 1e-05
MASKED_LOGIT = -100000.0
NORM_FLOOR = 0.1
MESH = pl.DeviceIdType.MESH
F32 = jnp.float32
BF16 = jnp.bfloat16
NN = (((1,), (0,)), ((), ()))
NT = (((1,), (1,)), ((), ()))
INDEX_AT = 12
MASK_AT = 13
PART = 32


def rotation_from(quat_b, quat_c, quat_d):
    inverse = 1.0 / (1.0 + quat_b * quat_b + quat_c * quat_c + quat_d * quat_d)
    entries = [
        1.0 + quat_b * quat_b - quat_c * quat_c - quat_d * quat_d,
        2.0 * (quat_b * quat_c - quat_d),
        2.0 * (quat_b * quat_d + quat_c),
        2.0 * (quat_b * quat_c + quat_d),
        1.0 - quat_b * quat_b + quat_c * quat_c - quat_d * quat_d,
        2.0 * (quat_c * quat_d - quat_b),
        2.0 * (quat_b * quat_d - quat_c),
        2.0 * (quat_c * quat_d + quat_b),
        1.0 - quat_b * quat_b - quat_c * quat_c + quat_d * quat_d,
    ]
    return [entry * inverse for entry in entries]


def layer_norm(values):
    center = values - jnp.mean(values, axis=-1, keepdims=True)
    spread = jnp.mean(center * center, axis=-1, keepdims=True)
    return center * lax.rsqrt(spread + NORM_EPSILON)


def split(x):
    high = x.astype(BF16)
    return high, (x - high.astype(F32)).astype(BF16)


def mm(a, b, dims=NN):
    return lax.dot_general(a, b, dims, preferred_element_type=F32)


def mm3(a, b, dims=NN):
    return mm(a[0], b[0], dims) + (mm(a[0], b[1], dims) + mm(a[1], b[0], dims))


def head_mask(width):
    head = lax.broadcasted_iota(jnp.int32, (HP, H * width), 0) * width
    lane = lax.broadcasted_iota(jnp.int32, (HP, H * width), 1)
    return ((lane >= head) & (lane < head + width)).astype(F32)


def spread_heads(rows, mask):
    return jnp.concatenate(
        [rows[i : i + 1] * mask for i in range(rows.shape[0])], axis=0
    )


def pick_heads(rows, mask):
    width = rows.shape[1]
    return jnp.sum(rows.reshape(-1, HP, width) * mask[None], axis=1)


def kernel(
    nrow,
    ncol,
    s0_ref,
    params_ref,
    shift_ref,
    index_ref,
    mask_ref,
    pair_ref,
    relpos_ref,
    gain_ref,
    bw_ref,
    hw_ref,
    ws_ref,
    wp_ref,
    wo_ref,
    wh_ref,
    wb_ref,
    wf_ref,
    single_ref,
    frames_ref,
    ws_in,
    wp_in,
    wo_in,
    wh_in,
    wb_in,
    state,
    outgoing,
    gathered,
    pairs,
    normed,
    bias,
    pair_out,
    wst,
    wpt,
    wo2,
    wh2,
    wb2,
    pair_send,
    pair_recv,
    pair_local,
    state_send,
    state_recv,
    weight_sem,
):
    n = nrow * ncol
    row = lax.axis_index("row")
    col = lax.axis_index("col")
    me = row * ncol + col
    owned = s0_ref.shape[0]
    count = n * owned
    col_rows = pair_ref.shape[1]

    barrier = pltpu.get_barrier_semaphore()

    def greet(k, carry):
        other = lax.rem(me + k, n)
        pl.semaphore_signal(
            barrier, inc=1, device_id=(other // ncol, lax.rem(other, ncol)), device_id_type=MESH
        )
        return carry

    lax.fori_loop(1, n, greet, 0)

    my_cols = pl.ds(pl.multiple_of(col * col_rows, col_rows), col_rows)

    def state_copy(step, k):
        other = lax.rem(me + k, n)
        return pltpu.make_async_remote_copy(
            src_ref=outgoing.at[step],
            dst_ref=gathered.at[step, me],
            send_sem=state_send.at[step],
            recv_sem=state_recv.at[step],
            device_id=(other // ncol, lax.rem(other, ncol)),
            device_id_type=MESH,
        )

    def send_state(step):
        def one(k, carry):
            state_copy(step, k).start()
            return carry

        lax.fori_loop(1, n, one, 0)

    def wait_all(step, sem):
        part = gathered.at[step, pl.ds(0, n - 1)]
        pltpu.make_async_copy(part, part, sem.at[step]).wait()

    loads = [
        pltpu.make_async_copy(source, target, weight_sem.at[at])
        for at, (source, target) in enumerate(
            ((ws_ref, ws_in), (wp_ref, wp_in), (wo_ref, wo_in), (wh_ref, wh_in), (wb_ref, wb_in))
        )
    ]
    for load in loads:
        load.start()
    eye = lax.broadcasted_iota(jnp.int32, (owned, owned), 0) == lax.broadcasted_iota(
        jnp.int32, (owned, owned), 1
    )

    def upright(line):
        return jnp.sum(jnp.where(eye, line, 0.0), axis=1, keepdims=True)

    quat = [upright(params_ref[a : a + 1]) for a in range(3)]
    start = rotation_from(*quat) + [upright(shift_ref[a : a + 1]) for a in range(3)]
    start += [upright(index_ref[...].astype(F32)), upright(mask_ref[...].astype(F32))]
    place = lax.broadcasted_iota(jnp.int32, (owned, WIDE - D), 1)
    first = jnp.zeros((owned, WIDE - D), F32)
    for k, entry in enumerate(start):
        first = jnp.where(place == k, entry, first)
    own_index = start[INDEX_AT]

    def post(step, values, block):
        high, low = split(block)
        rest = (block - high.astype(F32) - low.astype(F32)).astype(BF16)
        message = (
            high.astype(F32)
            + pltpu.roll(low.astype(F32), PART, 1)
            + pltpu.roll(rest.astype(F32), 2 * PART, 1)
        )
        for target in (outgoing.at[step], gathered.at[step, me]):
            target[:, :D] = values.astype(BF16)
            target[:, D:] = message.astype(BF16)

    state[0, :, :D] = s0_ref[...]
    state[0, :, D:] = first
    post(0, s0_ref[...], first)
    own_pair = pltpu.make_async_copy(
        pair_ref.at[pl.ds(col * owned, owned)], pairs.at[:, my_cols], pair_local
    )
    own_pair.start()
    pl.semaphore_wait(barrier, n - 1)
    send_state(0)
    for k in range(1, ncol):
        other = lax.rem(col + k, ncol)
        pltpu.make_async_remote_copy(
            src_ref=pair_ref.at[pl.ds(other * owned, owned)],
            dst_ref=pairs.at[:, my_cols],
            send_sem=pair_send,
            recv_sem=pair_recv,
            device_id=(row, other),
            device_id_type=MESH,
        ).start()

    for load, source, target in zip(
        loads, (ws_in, wp_in, wo_in, wh_in, wb_in), (wst, wpt, wo2, wh2, wb2)
    ):
        load.wait()
        high, low = split(source[...])
        target[0] = high
        target[1] = low
    heads = hw_ref[...]
    heads = jnp.maximum(heads, 0.0) + jnp.log1p(jnp.exp(-jnp.abs(heads)))
    heads = heads * (math.sqrt(2.0 / (9.0 * PQ)) / 2.0)
    here = lax.broadcasted_iota(jnp.int32, (HP, H), 0) == lax.broadcasted_iota(
        jnp.int32, (HP, H), 1
    )
    point_scale = jnp.concatenate(
        [jnp.sum(jnp.where(here, heads, 0.0), axis=1, keepdims=True)] * owned, axis=0
    )
    bias[...] = jnp.zeros_like(bias)

    own_pair.wait()
    if ncol > 1:
        part = pairs.at[:, pl.ds(0, (ncol - 1) * col_rows)]
        pltpu.make_async_copy(part, part, pair_recv).wait()
    wait_all(0, state_recv)

    blocks = gathered[0, :, :, D:].astype(F32).reshape(count, WIDE - D)
    index_col = sum(
        blocks[:, at : at + 1] for at in range(INDEX_AT, INDEX_AT + 3 * PART, PART)
    )
    lanes = lax.broadcasted_iota(jnp.int32, (count, BINS), 1).astype(F32)
    sublanes = lax.broadcasted_iota(jnp.int32, (owned, 1), 0)
    relpos = relpos_ref[...]
    gain = gain_ref[...]
    bw = bw_ref[...]

    def prepare(i, carry):
        mine = jnp.sum(jnp.where(sublanes == i, own_index, 0.0), axis=0, keepdims=True)
        offset = jnp.clip(index_col - mine, -(BINS // 2), BINS // 2 - 1) + BINS // 2
        onehot = (offset == lanes).astype(F32).astype(BF16)
        summed = pairs[i].astype(F32) + mm(onehot, relpos)
        rows = (layer_norm(summed) * gain).astype(BF16)
        normed[i] = rows
        bias[i, :H] = mm(bw, rows, NT)
        return carry

    lax.fori_loop(0, owned, prepare, 0)

    def dense(x, weight, begin, size):
        high, low = split(x)
        stacked = jnp.concatenate([high.astype(F32), low.astype(F32)], axis=0).astype(BF16)
        both = mm(stacked, weight[0, begin : begin + size])
        return both[:owned] + both[owned:] + mm(high, weight[1, begin : begin + size])

    def step_body(step, carry):
        @pl.when(step > 0)
        def _():
            wait_all(step, state_recv)

        turned = gathered[step].astype(F32).reshape(count, WIDE).T
        x = turned[:D].astype(BF16)
        joined = turned[D : D + 16] + (
            turned[D + PART : D + PART + 16] + turned[D + 2 * PART : D + 2 * PART + 16]
        )
        frame = [joined[k : k + 1] for k in range(14)]
        mine = state[step]
        own = mine[:, :D]
        block = mine[:, D:]
        rot = [block[:, k : k + 1] for k in range(9)]
        pos = [block[:, 9 + k : 10 + k] for k in range(3)]
        own2 = split(own)
        hc = H * C
        keyval = (mm(wst[0, hc:], x) + mm(wst[1, hc:], x)).astype(BF16)
        keys, values = keyval[:hc], keyval[hc:]
        kp = 3 * H * PQ
        locals_t = mm(wpt[0, kp:], x) + mm(wpt[1, kp:], x)

        def lift(base, width):
            p = [locals_t[base + a * width : base + (a + 1) * width] for a in range(3)]
            return [
                frame[3 * a] * p[0] + frame[3 * a + 1] * p[1] + frame[3 * a + 2] * p[2] + frame[9 + a]
                for a in range(3)
            ]

        key_points = lift(0, H * PQ)
        value_points = lift(kp, H * PV)
        query = mm3(own2, (wst[0, :hc], wst[1, :hc]), NT).astype(BF16).astype(F32)
        q = [
            mm3(
                own2,
                (
                    wpt[0, a * H * PQ : (a + 1) * H * PQ],
                    wpt[1, a * H * PQ : (a + 1) * H * PQ],
                ),
                NT,
            )
            for a in range(3)
        ]
        query_points = [
            rot[3 * a] * q[0] + rot[3 * a + 1] * q[1] + rot[3 * a + 2] * q[2] + pos[a]
            for a in range(3)
        ]
        mask_c, mask_q, mask_v = head_mask(C), head_mask(PQ), head_mask(PV)
        scores = mm(spread_heads(query, mask_c).astype(BF16), keys) * (1.0 / math.sqrt(C))
        cross = None
        query_square = None
        for a in range(3):
            wide = spread_heads(query_points[a], mask_q)
            term = mm3(split(wide), split(key_points[a]))
            square = jnp.sum(wide * wide, axis=-1, keepdims=True)
            cross = term if cross is None else cross + term
            query_square = square if query_square is None else query_square + square
        squares = (
            key_points[0] * key_points[0]
            + key_points[1] * key_points[1]
            + key_points[2] * key_points[2]
        )
        selector = jnp.concatenate([mask_q] * owned, axis=0).astype(BF16)
        square_high, square_low = split(squares)
        square_rest = (squares - square_high.astype(F32) - square_low.astype(F32)).astype(BF16)
        key_square = mm(selector, square_high) + (
            mm(selector, square_low) + mm(selector, square_rest)
        )
        distance = query_square + key_square - 2.0 * cross
        biases = bias[...].reshape(owned * HP, count)
        logits = math.sqrt(1.0 / 3.0) * (scores + biases - point_scale * distance)
        ones = jnp.ones((HP, 1), F32)
        live_row = jnp.concatenate(
            [block[i : i + 1, MASK_AT : MASK_AT + 1] * ones for i in range(owned)], axis=0
        )
        logits = jnp.where(live_row * frame[MASK_AT] > 0.5, logits, MASKED_LOGIT)
        top = jnp.max(logits, axis=-1, keepdims=True)
        weights = jnp.exp(logits - top)
        weights = weights * (1.0 / jnp.sum(weights, axis=-1, keepdims=True))
        weights2 = split(weights)
        rounded = weights2[0]
        scalar_out = pick_heads(mm(rounded, values, NT), mask_c)
        for i in range(owned):
            pair_out[i] = mm(rounded[i * HP : (i + 1) * HP], normed[i])
        moved = [
            pick_heads(mm3(weights2, split(value_points[a]), NT), mask_v) - pos[a]
            for a in range(3)
        ]
        local = [rot[a] * moved[0] + rot[3 + a] * moved[1] + rot[6 + a] * moved[2] for a in range(3)]
        lengths = jnp.sqrt(
            local[0] * local[0] + local[1] * local[1] + local[2] * local[2] + NORM_FLOOR
        )
        pv = H * PV
        mixed = dense(scalar_out, wo2, 0, hc)
        for a in range(3):
            mixed = mixed + dense(local[a], wo2, hc + a * pv, pv)
        mixed = mixed + dense(lengths, wo2, hc + 3 * pv, pv)
        pairs_flat = jnp.concatenate([pair_out[:, h, :] for h in range(H)], axis=-1)
        begin = hc + 4 * pv
        mixed = mixed + dense(pairs_flat, wo2, begin, H * BINS)
        single = layer_norm(own + mixed)
        hidden = jnp.maximum(dense(single, wh2, 0, D), 0.0)
        single = layer_norm(single + dense(hidden, wb2, 0, D))
        update = mm3(split(single), split(wf_ref[...]), NT)
        u = [update[:, k : k + 1] for k in range(6)]
        turn = rotation_from(u[0], u[1], u[2])
        new_rot = [
            rot[3 * a] * turn[b] + rot[3 * a + 1] * turn[3 + b] + rot[3 * a + 2] * turn[6 + b]
            for a in range(3)
            for b in range(3)
        ]
        new_pos = [
            rot[3 * a] * u[3] + rot[3 * a + 1] * u[4] + rot[3 * a + 2] * u[5] + pos[a]
            for a in range(3)
        ]
        packed = block
        for k, entry in enumerate(new_rot + new_pos):
            packed = jnp.where(place == k, entry, packed)
        state[step + 1, :, :D] = single
        state[step + 1, :, D:] = packed

        @pl.when(step < ITERS - 1)
        def _():
            post(step + 1, single, packed)
            send_state(step + 1)

        return carry

    lax.fori_loop(0, ITERS, step_body, 0)
    single_ref[...] = state[ITERS, :, :D]
    frames_ref[...] = state[ITERS, :, D:][:, :12]
    for step in range(ITERS):
        wait_all(step, state_send)
    if ncol > 1:
        part = pairs.at[:, pl.ds(0, (ncol - 1) * col_rows)]
        pltpu.make_async_copy(part, part, pair_send).wait()


def body(
    nrow,
    ncol,
    pair,
    relpos,
    pair_gain,
    bias_weight,
    single,
    rotation_params,
    translation,
    residue_index,
    residue_mask,
    w_scalar,
    w_points,
    head_weights,
    w_out,
    w_hidden,
    w_back,
    w_frame,
):
    owned = single.shape[0]
    count = owned * nrow * ncol
    channels = pair.shape[2]
    out_f = w_out.shape[0]
    vmem = pl.BlockSpec(memory_space=pltpu.VMEM)
    away = pl.BlockSpec(memory_space=pl.ANY)
    out, frames = pl.pallas_call(
        functools.partial(kernel, nrow, ncol),
        out_shape=(
            jax.ShapeDtypeStruct((owned, D), F32),
            jax.ShapeDtypeStruct((owned, 12), F32),
        ),
        in_specs=[vmem] * 10 + [away] * 5 + [vmem],
        out_specs=(vmem, vmem),
        scratch_shapes=[
            pltpu.VMEM((w_scalar.shape[1], D), F32),
            pltpu.VMEM((w_points.shape[1], D), F32),
            pltpu.VMEM((out_f, D), F32),
            pltpu.VMEM((D, D), F32),
            pltpu.VMEM((D, D), F32),
            pltpu.VMEM((ITERS + 1, owned, WIDE), F32),
            pltpu.VMEM((ITERS, owned, WIDE), BF16),
            pltpu.VMEM((ITERS, count // owned, owned, WIDE), BF16),
            pltpu.VMEM((owned, count, channels), BF16),
            pltpu.VMEM((owned, count, channels), BF16),
            pltpu.VMEM((owned, HP, count), F32),
            pltpu.VMEM((owned, HP, channels), F32),
            pltpu.VMEM((2, w_scalar.shape[1], D), BF16),
            pltpu.VMEM((2, w_points.shape[1], D), BF16),
            pltpu.VMEM((2, out_f, D), BF16),
            pltpu.VMEM((2, D, D), BF16),
            pltpu.VMEM((2, D, D), BF16),
            pltpu.SemaphoreType.DMA,
            pltpu.SemaphoreType.DMA,
            pltpu.SemaphoreType.DMA,
            pltpu.SemaphoreType.DMA((ITERS,)),
            pltpu.SemaphoreType.DMA((ITERS,)),
            pltpu.SemaphoreType.DMA((5,)),
        ],
        compiler_params=pltpu.CompilerParams(
            collective_id=0, has_side_effects=True, vmem_limit_bytes=58 * 1024 * 1024
        ),
    )(
        single,
        rotation_params,
        translation,
        residue_index[None],
        residue_mask[None],
        pair,
        relpos,
        pair_gain[None],
        bias_weight.T,
        head_weights[None],
        w_scalar.T,
        w_points.T,
        w_out,
        w_hidden,
        w_back,
        w_frame.T,
    )
    return out, frames.T


def solution(mesh):
    placed = (
        P("row", "col", None),
        P(),
        P(),
        P(),
        P(("row", "col"), None),
        P(None, ("row", "col")),
        P(None, ("row", "col")),
        P(("row", "col")),
        P(("row", "col")),
        P(),
        P(),
        P(),
        P(),
        P(),
        P(),
        P(),
    )
    return jax.shard_map(
        functools.partial(body, mesh.shape["row"], mesh.shape["col"]),
        mesh=mesh,
        in_specs=placed,
        out_specs=(P(("row", "col"), None), P(None, ("row", "col"))),
        check_vma=False,
    )
```
